32 devices in a mesh: front: 4 (over x, core), grid: 8 (over z, y).
Axes of the slice: x: 2, y: 2, z: 4, core: 2. Of those that a mesh axis runs over, the one named last changes fastest.
Arguments:
- index_map: int32 [4, 8192], P('front'), may hold values from 0 to 16383, as said below
- lengths: int32 [4], P('front'), may hold values from 1 to 8192, 24576 in all
- update_front: float32 [4, 8192, 8192], P('front', 'grid'), may hold values from -0.0625 to 0.0625
- front_matrix: float32 [16384, 16384], P(('front', 'grid')), may hold values from -0.046875 to 0.046875
- random: float32 [16384, 256], P(('front', 'grid')), may hold values from -6 to 6
Outputs:
- parent_sample: float32 [16384, 256], P(('front', 'grid'))
The draws below stay inside these ranges and needn't reach their ends.
Inputs may be any that keep to these rules, and one draw needn't show every extreme that they name: `index_map`: within one child the 8192 entries are distinct parent rows. `lengths`: rows of a child at or past its length are not live; the largest length equals 8192.
All inputs are finite; a program needn't handle non-finite values. No bound on the sum of `lengths` on one device may be relied on, other than what follows from the above.
Results may differ from the reference program's by a relative error of at most 0.0003.
Values sent between devices are 32-bit elements; how exact they have to be, the bound alone decides.
A program may use at most 192 MiB of HBM per device.

```python
import math
import jax
import jax.numpy as jnp
import numpy as np
from jax import lax

WP = 16384
UC = 8192
K = 256
CHILDREN = 4


def draw_index_map(key, part):
    child_keys = jax.random.split(jax.random.fold_in(key, 17), CHILDREN)
    picked = jax.vmap(lambda child_key: jax.random.permutation(child_key, WP)[:UC])(child_keys)
    return picked.astype(jnp.int32)


def levels(stream_key, shape, shards, smallest, largest):
    factor_of, own = 1.0, jax.random.fold_in(stream_key, 6)
    for position, shards_of in shards:
        heights = jnp.exp(jax.random.uniform(jax.random.fold_in(own, position), (shards_of,), jnp.float32, smallest / len(shards), largest / len(shards)))
        factor_of = factor_of * jnp.repeat(heights, shape[position] // shards_of).reshape([-1 if axis == position else 1 for axis in range(len(shape))])
    return factor_of


def length_profile(count, total, bound, skew):
    portions = [(1 << 20) // math.isqrt(standing ** skew) + 1 for standing in range(2, count + 1)]
    rest, holding = total - bound - (count - 1), [1] * (count - 1)
    while rest > 0:
        candidates = [i for i in range(count - 1) if holding[i] < bound]
        mass, remaining = sum([portions[i] for i in candidates]), rest
        for i in candidates:
            addition = min(bound - holding[i], max(1, remaining * portions[i] // mass), rest)
            holding[i] = holding[i] + addition
            rest = rest - addition
    return np.array([bound] + holding)


def ragged_sizes(stream_key, amount, total, reach, skew):
    if amount == 2:
        one = jax.random.randint(stream_key, (), max(1, total - reach), min(reach, total - 1) + 1)
        return jnp.stack([one, total - one])
    sizes = jnp.asarray(length_profile(amount, total, reach, skew), jnp.int32)
    twos = (amount - 1) // 2
    source_of, receiver = sizes[1:1 + 2 * twos:2], sizes[2:2 + 2 * twos:2]
    room = jnp.minimum(source_of - 1, reach - receiver)
    shifted = jax.random.randint(jax.random.fold_in(stream_key, 1), (twos,), 0, 1 << 20) % (room + 1)
    sizes = sizes.at[1:1 + 2 * twos:2].set(source_of - shifted).at[2:2 + 2 * twos:2].set(receiver + shifted)
    return sizes[jax.random.permutation(jax.random.fold_in(stream_key, 2), amount)]


def gaussian(key, dims, width, most, pieces=(), held_as=jnp.bfloat16):
    loudness = levels(key, dims, pieces, -0.22, 0.18) if pieces else 1.0
    drawn = jax.random.normal(key, dims, jnp.float32) * width * loudness
    return jnp.minimum(jnp.maximum(drawn, -most), most).astype(held_as)


def setup_inputs(seed: int = 0) -> dict:
    splits = jax.random.split(jax.random.key(seed), 6)
    return {
        "index_map": draw_index_map(jax.random.fold_in(splits[5], 71), 0),
        "lengths": ragged_sizes(splits[1], CHILDREN, 3 * UC, UC, 2).astype(jnp.int32),
        "update_front": gaussian(splits[2], (CHILDREN, UC, UC), UC ** -0.5, 0.0625, ((0, 4), (1, 8)), jnp.float32),
        "front_matrix": gaussian(splits[3], (WP, WP), WP ** -0.5, 0.046875, ((0, 32),), jnp.float32),
        "random": gaussian(splits[4], (WP, K), 1.0, 6.0, ((0, 32),), jnp.float32),
    }


def reference(index_map, lengths, update_front, front_matrix, random):
    parent_sample = jnp.dot(front_matrix, random, preferred_element_type=jnp.float32, precision=lax.Precision.HIGHEST)
    row_numbers = jnp.arange(UC, dtype=jnp.int32)

    def one_child(packed):
        child_rows, child_length, child_block = packed
        child_random = jnp.take(random, child_rows, axis=0)
        child_sample = jnp.dot(child_block, child_random, preferred_element_type=jnp.float32, precision=lax.Precision.HIGHEST)
        return jnp.where((row_numbers < child_length)[:, None], child_sample, jnp.float32(0.0))

    samples = lax.map(one_child, (index_map, lengths, update_front))
    for child in range(CHILDREN):
        parent_sample = parent_sample.at[index_map[child]].add(samples[child])
    return parent_sample
```

```python
import functools
import itertools
import math

import jax
import jax.numpy as jnp
from jax import lax
from jax.experimental import pallas as pl
from jax.experimental.pallas import tpu as pltpu
from jax.sharding import PartitionSpec as P

MESH = pl.DeviceIdType.MESH


def axis_dims(places):
    found = []
    for d in range(len(places[0])):
        values = [p[d] for p in places]
        size = len(set(values))
        if size > 1:
            stride = next(i for i, v in enumerate(values) if v != values[0])
            found.append((stride, size))
    found.sort(reverse=True)
    if math.prod(size for _, size in found) != len(places):
        found = [(1, len(places))]
    return found


class Plan:
    def __init__(self, mesh):
        self.front, self.grid = mesh.shape["front"], mesh.shape["grid"]
        place = lambda d: (*d.coords, d.core_on_chip)
        fronts = axis_dims([place(d) for d in mesh.devices[:, 0]])
        grids = axis_dims([place(d) for d in mesh.devices[0, :]])
        self.core = fronts[-1] if fronts[-1][1] == 2 else (1, 1)
        if self.core[1] == 2:
            fronts = fronts[:-1]
        dims = [("front", s, n) for s, n in fronts] + [("grid", s, n) for s, n in grids]
        long = max(range(len(dims)), key=lambda i: dims[i][2])
        rest = [i for i in range(len(dims)) if i != long]
        self.dims = dims
        a, b = rest, rest[::-1]
        if len(rest) == 2:
            self.orders = [(a[0], long, a[1]), (b[0], long, b[1]), (long, *a), (long, *b)]
        else:
            self.orders = [(*a, long), (long, *b)]
        self.items = self.schedule()

    def steps(self, offset, order):
        last = max((i for i, d in enumerate(order) if offset[d]), default=-1)
        moves = []
        if last >= 0 and self.dims[order[last]][2] > 2:
            moves.append((order[last], 1 if offset[order[last]] > 0 else -1))
        for d in order[last + 1 :]:
            moves += [(d, 1)] if self.dims[d][2] == 2 else [(d, 1), (d, -1)]
        return moves

    def schedule(self):
        spans = [range(2) if n == 2 else range(1 - n, n) for _, _, n in self.dims]
        items = []
        for offset in itertools.product(*spans):
            for color, order in enumerate(self.orders):
                stage = max((i for i, d in enumerate(order) if offset[d]), default=-1)
                items.append((sum(map(abs, offset)), stage, color, offset))
        items.sort()
        return [(color, offset) for hops, _, color, offset in items if hops]


def gather_rows(plan, x_ref, buf, own_sem, send, side_send, recv, side_recv, between=lambda: None):
    f, g = lax.axis_index("front"), lax.axis_index("grid")
    rows = x_ref.shape[0]
    colors = len(plan.orders)
    part = rows // colors
    at = [lax.rem((f if axis == "front" else g) // s, n) for axis, s, n in plan.dims]
    sibling = (f + 1 - 2 * lax.rem(f, 2), g)

    def moved(d, step):
        axis, stride, n = plan.dims[d]
        move = (1 - 2 * at[d]) if n == 2 else step
        return (f + move * stride, g) if axis == "front" else (f, g + move * stride)

    def inside(d, step):
        n = plan.dims[d][2]
        if n == 2:
            return None
        return at[d] + step <= n - 1 if step > 0 else at[d] + step >= 0

    def guarded(conditions, body):
        conditions = [c for c in conditions if c is not None]
        if conditions:
            pl.when(functools.reduce(jnp.logical_and, conditions))(body)
        else:
            body()

    def piece(ref, first, color):
        return ref.at[pl.ds(pl.multiple_of(first + color * part, 8), part)]

    def lane(d, step):
        return 2 * d + (step < 0)

    def remote(source, target, first, color, send_sem, recv_sem, device):
        return pltpu.make_async_remote_copy(
            src_ref=source, dst_ref=piece(target, first, color), send_sem=send_sem, recv_sem=recv_sem,
            device_id=device, device_id_type=MESH,
        )

    me = f * plan.grid + g
    seat = lambda ff, gg: (ff // plan.core[1]) * plan.grid + gg

    def pass_on(color, source, owner_f, owner_g, moves, conditions):
        first = (owner_f * plan.grid + owner_g) * rows
        for d, step in moves:
            def go(d=d, step=step):
                remote(
                    source, buf, first, color, send.at[lane(d, step), color, seat(owner_f, owner_g)],
                    recv.at[color, seat(owner_f, owner_g)], moved(d, step),
                ).start()
            guarded([inside(d, step)], go)

    own = pltpu.make_async_copy(x_ref, buf.at[pl.ds(pl.multiple_of(me * rows, 8), rows)], own_sem)
    own.start()
    zero = (0,) * len(plan.dims)
    for stage in range(len(plan.dims)):
        for color, order in enumerate(plan.orders):
            moves = [m for m in plan.steps(zero, order) if m[0] == order[stage]]
            pass_on(color, piece(x_ref, 0, color), f, g, moves, [])
    if plan.core[1] == 2:
        for color in range(colors):
            remote(
                piece(x_ref, 0, color), buf, me * rows, color, side_send.at[color, seat(f, g)],
                side_recv.at[color, seat(f, g)], sibling,
            ).start()

    between()

    def owner_of(offset):
        owner_f, owner_g, conditions = f, g, []
        for d, (axis, stride, n) in enumerate(plan.dims):
            if not offset[d]:
                continue
            move = (1 - 2 * at[d]) if n == 2 else -offset[d]
            if n > 2:
                conditions.append(at[d] - offset[d] >= 0 if offset[d] > 0 else at[d] - offset[d] <= n - 1)
            if axis == "front":
                owner_f = owner_f + move * stride
            else:
                owner_g = owner_g + move * stride
        return owner_f, owner_g, conditions

    for color, offset in plan.items:
        owner_f, owner_g, conditions = owner_of(offset)

        def arrive(color=color, offset=offset, owner_f=owner_f, owner_g=owner_g):
            first = (owner_f * plan.grid + owner_g) * rows
            here = piece(buf, first, color)
            remote(here, buf, first, color, send.at[0, color, seat(f, g)], recv.at[color, seat(owner_f, owner_g)], sibling).wait_recv()
            pass_on(color, here, owner_f, owner_g, plan.steps(offset, plan.orders[color]), conditions)
            if plan.core[1] == 2:
                remote(
                    here, buf, first, color, side_send.at[color, seat(owner_f, owner_g)],
                    side_recv.at[color, seat(owner_f, owner_g)], sibling,
                ).start()

        guarded(conditions, arrive)

    def finish():
        own.wait()
        everything = [(color, zero) for color in range(colors)] + plan.items
        for color, offset in everything:
            owner_f, owner_g, conditions = owner_of(offset)

            def settle(color=color, offset=offset, owner_f=owner_f, owner_g=owner_g):
                first = (owner_f * plan.grid + owner_g) * rows
                here = piece(buf, first, color)
                for d, step in plan.steps(offset, plan.orders[color]):
                    def gone(d=d, step=step):
                        remote(
                            here, buf, first, color, send.at[lane(d, step), color, seat(owner_f, owner_g)],
                            recv.at[color, seat(owner_f, owner_g)], moved(d, step),
                        ).wait_send()
                    guarded([inside(d, step)], gone)
                if plan.core[1] == 2:
                    remote(
                        here, buf, first, color, side_send.at[color, seat(owner_f, owner_g)],
                        side_recv.at[color, seat(owner_f, owner_g)], sibling,
                    ).wait_send()
                    theirs = ((owner_f + 1 - 2 * lax.rem(owner_f, 2)) * plan.grid + owner_g) * rows
                    remote(
                        piece(buf, theirs, color), buf, theirs, color, side_send.at[color, seat(owner_f, owner_g)],
                        side_recv.at[color, seat(owner_f, owner_g)], sibling,
                    ).wait_recv()

            guarded(conditions, settle)

    return finish


def greet(plan, everyone=False):
    f, g = lax.axis_index("front"), lax.axis_index("grid")
    bar = pltpu.get_barrier_semaphore()
    if everyone:
        total = plan.front * plan.grid
        me = f * plan.grid + g
        def hello(i, c):
            t = lax.rem(me + i, total)
            pl.semaphore_signal(bar, inc=1, device_id=(t // plan.grid, lax.rem(t, plan.grid)), device_id_type=MESH)
            return c
        lax.fori_loop(1, total, hello, 0)
        pl.semaphore_wait(bar, total - 1)


def ag_scratch(plan):
    seats = plan.front * plan.grid // plan.core[1]
    colors = len(plan.orders)
    return [
        pltpu.SemaphoreType.DMA(()),
        pltpu.SemaphoreType.DMA((2 * len(plan.dims), colors, seats)),
        pltpu.SemaphoreType.DMA((colors, seats)),
        pltpu.SemaphoreType.DMA((colors, seats)),
        pltpu.SemaphoreType.DMA((colors, seats)),
    ]


def halves(a):
    high = a.astype(jnp.bfloat16)
    return high, (a - high.astype(jnp.float32)).astype(jnp.bfloat16)


def dot(a, b):
    return jnp.dot(a, b, preferred_element_type=jnp.float32)


def add_product(acc, a_ref, high, low, tile):
    for m in range(a_ref.shape[0] // tile):
        rows = pl.ds(m * tile, tile)
        a_high, a_low = halves(a_ref[rows, :])
        acc[rows, :] += dot(a_high, high) + (dot(a_low, high) + dot(a_high, low))


def flat(block):
    return jnp.concatenate([block[:, 0, :], block[:, 1, :]], axis=1)


class Mail:
    def __init__(self, plan, rows, own_rows):
        self.plan, self.rows, self.own_rows = plan, rows, own_rows
        self.devices = plan.front * plan.grid
        mean = rows / self.devices
        self.slots = max(8, math.ceil((mean + 4.2 * math.sqrt(mean)) / 8) * 8)
        self.total = self.devices * self.slots
        self.parts = next(p for p in (4, 2, 1) if self.total % (16 * p) == 0)
        self.part = self.total // self.parts

    def scratch(self):
        return [
            pltpu.VMEM((self.devices, self.rows), jnp.float32),
            pltpu.VMEM((1, self.rows), jnp.float32),
            pltpu.VMEM((self.total, 1), jnp.float32),
            pltpu.VMEM((self.rows, 512), jnp.bfloat16),
            pltpu.VMEM((self.total, 256), jnp.float32),
            pltpu.VMEM((self.total, 256), jnp.float32),
            pltpu.SemaphoreType.DMA(()),
            pltpu.SemaphoreType.DMA((self.devices,)),
            pltpu.SemaphoreType.DMA((self.devices,)),
        ]

    def address(self, where, shift, peak, key, slot, target):
        n, rows, own = self.devices, self.rows, self.own_rows
        me = lax.axis_index("front") * self.plan.grid + lax.axis_index("grid")
        before = lax.broadcasted_iota(jnp.int32, (rows, rows), 0) < lax.broadcasted_iota(jnp.int32, (rows, rows), 1)
        before = jnp.where(before, 1.0, 0.0).astype(jnp.bfloat16)
        block = lax.broadcasted_iota(jnp.int32, (n, rows), 0)
        mine = where[pl.ds(me, 1), :]
        sent = (mine >= block * own) & (mine < (block + 1) * own)
        places = where[...] - me * own
        got = (places >= 0) & (places < own)
        both = jnp.concatenate([jnp.where(sent, 1.0, 0.0), jnp.where(got, 1.0, 0.0)], axis=0)
        rank = dot(both.astype(jnp.bfloat16), before) - shift
        own_rank, got_rank = rank[:n], rank[n:]
        fits = sent & (own_rank >= 0) & (own_rank < self.slots)
        number = (block * self.slots).astype(jnp.float32) + own_rank + 1.0
        slot[...] = jnp.sum(jnp.where(fits, number, 0.0), axis=0, keepdims=True) - 1.0
        key[...] = jnp.where(got, got_rank, -1.0)
        counter = lax.broadcasted_iota(jnp.int32, (self.slots, rows), 0).astype(jnp.float32)
        first = (block * own)

        def one(s, most):
            which = where[pl.ds(s, 1), :]
            held = counter == key[pl.ds(s, 1), :]
            place = (which - me * own + 1).astype(jnp.float32)
            found = jnp.sum(jnp.where(held, place, 0.0), axis=1, keepdims=True) - 1.0
            target[pl.ds(pl.multiple_of(s * self.slots, 8), self.slots), :] = found
            inside = (which >= first) & (which < first + own)
            return jnp.maximum(most, jnp.sum(jnp.where(inside, 1.0, 0.0), axis=1, keepdims=True))

        most = lax.fori_loop(0, n, one, jnp.zeros((n, 1), jnp.float32))
        if peak is not None:
            peak[...] = jnp.broadcast_to(jnp.max(most, axis=0, keepdims=True), peak.shape)

    def pack(self, slot, pair, out):
        def one(p, c):
            base = p * self.part
            ids = (lax.broadcasted_iota(jnp.int32, (self.part, self.rows), 0) + base).astype(jnp.float32)
            chosen = jnp.where(ids == slot[...], 1.0, 0.0).astype(jnp.bfloat16)
            both = dot(chosen, pair[...])
            out[pl.ds(pl.multiple_of(base, 8), self.part), :] = both[:, :256] + both[:, 256:]
            return c
        lax.fori_loop(0, self.parts, one, 0)

    def peer(self, i):
        me = lax.axis_index("front") * self.plan.grid + lax.axis_index("grid")
        return lax.rem(me + i, self.devices)

    def letter(self, i, out, inbox, sent, received):
        t = self.peer(i)
        me = self.peer(0)
        rows = lambda ref, b: ref.at[pl.ds(pl.multiple_of(b * self.slots, 8), self.slots)]
        return pltpu.make_async_remote_copy(
            src_ref=rows(out, t), dst_ref=rows(inbox, me), send_sem=sent.at[i],
            recv_sem=received.at[i], device_id=(t // self.plan.grid, lax.rem(t, self.plan.grid)),
            device_id_type=MESH,
        )

    def home(self, out, inbox, sem):
        me = self.peer(0)
        rows = lambda ref: ref.at[pl.ds(pl.multiple_of(me * self.slots, 8), self.slots)]
        return pltpu.make_async_copy(rows(out), rows(inbox), sem)

    def send(self, out, inbox, sem, sent, received):
        self.home(out, inbox, sem).start()

        def one(i, c):
            self.letter(i, out, inbox, sent, received).start()
            return c
        lax.fori_loop(1, self.devices, one, 0)

    def settle(self, out, inbox, sem, sent, received):
        def one(i, c):
            self.letter(i, out, inbox, sent, received).wait()
            return c
        lax.fori_loop(1, self.devices, one, 0)
        self.home(out, inbox, sem).wait()

    def unpack(self, target, inbox, acc):
        def one(p, c):
            rows = pl.ds(pl.multiple_of(p * self.part, 8), self.part)
            places = lax.broadcasted_iota(jnp.int32, (self.part, self.own_rows), 1).astype(jnp.float32)
            chosen = jnp.where(target[rows, :] == places, 1.0, 0.0).astype(jnp.bfloat16)
            pair = jnp.concatenate(halves(inbox[rows, :]), axis=1)
            both = lax.dot_general(chosen, pair, (((0,), (0,)), ((), ())), preferred_element_type=jnp.float32)
            acc[...] += both[:, :256] + both[:, 256:]
            return c
        lax.fori_loop(0, self.parts, one, 0)


def main_kernel(plan, mail, index, live, x, u_hbm, f_hbm, out, sample, peak, rest_out, rows_all, where, child, ubuf,
                fbuf, acc, total, usem, fsem, wsem, wsend, wrecv, ssem, *more):
    ag, post = more[:5], more[5:]
    key, slot, target, pair, outbox, inbox, msem, sent, received = post
    f, g = lax.axis_index("front"), lax.axis_index("grid")
    greet(plan, True)
    depth, wide = child.shape[1], fbuf.shape[2]
    u_steps, f_steps = u_hbm.shape[1] // depth, f_hbm.shape[1] // wide
    slots = ubuf.shape[0]

    def u_copy(k):
        s = lax.rem(k, slots)
        return pltpu.make_async_copy(u_hbm.at[:, pl.ds(pl.multiple_of(k * depth, depth), depth)], ubuf.at[s], usem.at[s])

    def f_copy(k):
        s = lax.rem(k, slots)
        return pltpu.make_async_copy(f_hbm.at[:, pl.ds(pl.multiple_of(k * wide, wide), wide)], fbuf.at[s], fsem.at[s])

    block = plan.grid
    def here(ref, ff):
        return ref.at[pl.ds(pl.multiple_of(ff * block, 8), block)]
    def exchange(i):
        return pltpu.make_async_remote_copy(
            src_ref=live, dst_ref=here(where, f), send_sem=wsend.at[i], recv_sem=wrecv.at[i],
            device_id=(lax.rem(f + i, plan.front), g), device_id_type=MESH,
        )
    for i in range(1, plan.front):
        exchange(i).start()
    mine = pltpu.make_async_copy(live, here(where, f), wsem)
    mine.start()
    for k in range(slots):
        u_copy(k).start()
        f_copy(k).start()

    def between():
        for i in range(1, plan.front):
            exchange(i).wait()
        mine.wait()
        mail.address(where, 0.0, peak, key, slot, target)

    finish = gather_rows(plan, x, rows_all, *ag, between=between)
    finish()

    acc[...] = jnp.zeros_like(acc)

    def u_step(k, c):
        u_copy(k).wait()
        def fetch(j, c):
            for t in range(16):
                r = j * 16 + t
                child[0, r] = rows_all[index[k * depth + r]]
            return c
        lax.fori_loop(0, depth // 16, fetch, 0)
        high, low = halves(flat(child[0]))
        add_product(acc, ubuf.at[lax.rem(k, slots)], high, low, 256)
        @pl.when(k + slots < u_steps)
        def _():
            u_copy(k + slots).start()
        return c
    lax.fori_loop(0, u_steps, u_step, 0)

    pair[...] = jnp.concatenate(halves(acc[...]), axis=1)
    mail.pack(slot, pair, outbox)
    keep = pltpu.make_async_copy(acc, sample, ssem)
    keep.start()
    mail.send(outbox, inbox, msem, sent, received)

    total[...] = jnp.zeros_like(total)

    def f_step(k, c):
        f_copy(k).wait()
        high, low = halves(flat(rows_all[pl.ds(pl.multiple_of(k * wide, wide), wide)]))
        add_product(total, fbuf.at[lax.rem(k, slots)], high, low, min(256, fbuf.shape[1]))
        @pl.when(k + slots < f_steps)
        def _():
            f_copy(k + slots).start()
        return c
    lax.fori_loop(0, f_steps, f_step, 0)

    mail.settle(outbox, inbox, msem, sent, received)
    mail.unpack(target, inbox, total)
    out[...] = total[...]
    copy = pltpu.make_async_copy(where, rest_out, wsem)
    copy.start()
    copy.wait()
    keep.wait()


def extra_kernel(plan, mail, shift, where, sample, so_far, out, pair, *post):
    key, slot, target, pair2, outbox, inbox, msem, sent, received = post
    greet(plan, True)
    mail.address(where, shift[0:1, 0:1], None, key, slot, target)
    pair2[...] = jnp.concatenate(halves(sample[...]), axis=1)
    mail.pack(slot, pair2, outbox)
    mail.send(outbox, inbox, msem, sent, received)
    pair[...] = so_far[...]
    mail.settle(outbox, inbox, msem, sent, received)
    mail.unpack(target, inbox, pair)
    out[...] = pair[...]


def shards(plan, index_map, lengths, update_front, front_matrix, random):
    order, own_rows = index_map.shape[1], front_matrix.shape[0]
    rows, width = update_front.shape[1], random.shape[1]
    mail = Mail(plan, rows, own_rows)
    index = index_map[0]
    live = jnp.where(jnp.arange(order, dtype=jnp.int32) < lengths[0], index, -1).reshape(plan.grid, rows)
    x = random.reshape(own_rows, 2, width // 2)
    depth, wide, slots = 512, 1024, 3
    vmem, any_ = pl.BlockSpec(memory_space=pltpu.VMEM), pl.BlockSpec(memory_space=pl.ANY)
    devices = plan.front * plan.grid
    first, sample, peak, where = pl.pallas_call(
        functools.partial(main_kernel, plan, mail),
        out_shape=(
            jax.ShapeDtypeStruct((own_rows, width), jnp.float32),
            jax.ShapeDtypeStruct((rows, width), jnp.float32),
            jax.ShapeDtypeStruct((8, 128), jnp.float32),
            jax.ShapeDtypeStruct((devices, rows), jnp.int32),
        ),
        in_specs=[pl.BlockSpec(memory_space=pltpu.SMEM), vmem, vmem, any_, any_],
        out_specs=(vmem, any_, vmem, any_),
        scratch_shapes=[
            pltpu.VMEM((own_rows * devices, 2, width // 2), jnp.float32),
            pltpu.VMEM((devices, rows), jnp.int32),
            pltpu.VMEM((2, depth, 2, width // 2), jnp.float32),
            pltpu.VMEM((slots, rows, depth), jnp.float32),
            pltpu.VMEM((slots, own_rows, wide), jnp.float32),
            pltpu.VMEM((rows, width), jnp.float32),
            pltpu.VMEM((own_rows, width), jnp.float32),
            pltpu.SemaphoreType.DMA((slots,)),
            pltpu.SemaphoreType.DMA((slots,)),
            pltpu.SemaphoreType.DMA(()),
            pltpu.SemaphoreType.DMA((plan.front,)),
            pltpu.SemaphoreType.DMA((plan.front,)),
            pltpu.SemaphoreType.DMA(()),
            *ag_scratch(plan),
            *mail.scratch(),
        ],
        compiler_params=pltpu.CompilerParams(collective_id=0, has_side_effects=True, vmem_limit_bytes=63 << 20),
    )(index, live, x, update_front[0], front_matrix)

    def more(carry):
        done, so_far = carry
        shift = jnp.full((8, 128), done, jnp.float32)
        added = pl.pallas_call(
            functools.partial(extra_kernel, plan, mail),
            out_shape=jax.ShapeDtypeStruct((own_rows, width), jnp.float32),
            in_specs=[vmem] * 4,
            out_specs=vmem,
            scratch_shapes=[pltpu.VMEM((own_rows, width), jnp.float32), *mail.scratch()],
            compiler_params=pltpu.CompilerParams(collective_id=1, has_side_effects=True, vmem_limit_bytes=63 << 20),
        )(shift, where, sample, so_far)
        return done + mail.slots, added

    return lax.while_loop(lambda carry: carry[0] < peak[0, 0], more, (jnp.float32(mail.slots), first))[1]


def solution(mesh):
    plan = Plan(mesh)
    placed = (
        P("front", None),
        P("front"),
        P("front", "grid", None),
        P(("front", "grid"), None),
        P(("front", "grid"), None),
    )
    return jax.shard_map(
        functools.partial(shards, plan), mesh=mesh, in_specs=placed, out_specs=P(("front", "grid"), None),
        check_vma=False,
    )
```

```python
import functools
import itertools
import math

import jax
import jax.numpy as jnp
from jax import lax
from jax.experimental import pallas as pl
from jax.experimental.pallas import tpu as pltpu
from jax.sharding import PartitionSpec as P

MESH = pl.DeviceIdType.MESH


def axis_dims(places):
    found = []
    for d in range(len(places[0])):
        values = [p[d] for p in places]
        size = len(set(values))
        if size > 1:
            stride = next(i for i, v in enumerate(values) if v != values[0])
            found.append((stride, size))
    found.sort(reverse=True)
    if math.prod(size for _, size in found) != len(places):
        found = [(1, len(places))]
    return found


class Plan:
    def __init__(self, mesh):
        self.front, self.grid = mesh.shape["front"], mesh.shape["grid"]
        place = lambda d: (*d.coords, d.core_on_chip)
        fronts = axis_dims([place(d) for d in mesh.devices[:, 0]])
        grids = axis_dims([place(d) for d in mesh.devices[0, :]])
        self.core = fronts[-1] if fronts[-1][1] == 2 else (1, 1)
        if self.core[1] == 2:
            fronts = fronts[:-1]
        dims = [("front", s, n) for s, n in fronts] + [("grid", s, n) for s, n in grids]
        long = max(range(len(dims)), key=lambda i: dims[i][2])
        rest = [i for i in range(len(dims)) if i != long]
        self.dims = dims
        a, b = rest, rest[::-1]
        if len(rest) == 2:
            self.orders = [(a[0], long, a[1]), (b[0], long, b[1]), (long, *a), (long, *b)]
        else:
            self.orders = [(*a, long), (long, *b)]
        self.items = self.schedule()

    def steps(self, offset, order):
        last = max((i for i, d in enumerate(order) if offset[d]), default=-1)
        moves = []
        if last >= 0 and self.dims[order[last]][2] > 2:
            moves.append((order[last], 1 if offset[order[last]] > 0 else -1))
        for d in order[last + 1 :]:
            moves += [(d, 1)] if self.dims[d][2] == 2 else [(d, 1), (d, -1)]
        return moves

    def schedule(self):
        spans = [range(2) if n == 2 else range(1 - n, n) for _, _, n in self.dims]
        items = []
        for offset in itertools.product(*spans):
            for color, order in enumerate(self.orders):
                stage = max((i for i, d in enumerate(order) if offset[d]), default=-1)
                items.append((sum(map(abs, offset)), stage, color, offset))
        items.sort()
        return [(color, offset) for hops, _, color, offset in items if hops]


def gather_rows(plan, x_ref, buf, own_sem, send, side_send, recv, side_recv, between=lambda: None, chores=()):
    f, g = lax.axis_index("front"), lax.axis_index("grid")
    rows = x_ref.shape[0]
    colors = len(plan.orders)
    part = rows // colors
    at = [lax.rem((f if axis == "front" else g) // s, n) for axis, s, n in plan.dims]
    sibling = (f + 1 - 2 * lax.rem(f, 2), g)

    def moved(d, step):
        axis, stride, n = plan.dims[d]
        move = (1 - 2 * at[d]) if n == 2 else step
        return (f + move * stride, g) if axis == "front" else (f, g + move * stride)

    def inside(d, step):
        n = plan.dims[d][2]
        if n == 2:
            return None
        return at[d] + step <= n - 1 if step > 0 else at[d] + step >= 0

    def guarded(conditions, body):
        conditions = [c for c in conditions if c is not None]
        if conditions:
            pl.when(functools.reduce(jnp.logical_and, conditions))(body)
        else:
            body()

    def piece(ref, first, color):
        return ref.at[pl.ds(pl.multiple_of(first + color * part, 8), part)]

    def lane(d, step):
        return 2 * d + (step < 0)

    def remote(source, target, first, color, send_sem, recv_sem, device):
        return pltpu.make_async_remote_copy(
            src_ref=source, dst_ref=piece(target, first, color), send_sem=send_sem, recv_sem=recv_sem,
            device_id=device, device_id_type=MESH,
        )

    me = f * plan.grid + g
    seat = lambda ff, gg: (ff // plan.core[1]) * plan.grid + gg

    def pass_on(color, source, owner_f, owner_g, moves, conditions):
        first = (owner_f * plan.grid + owner_g) * rows
        for d, step in moves:
            def go(d=d, step=step):
                remote(
                    source, buf, first, color, send.at[lane(d, step), color, seat(owner_f, owner_g)],
                    recv.at[color, seat(owner_f, owner_g)], moved(d, step),
                ).start()
            guarded([inside(d, step)], go)

    own = pltpu.make_async_copy(x_ref, buf.at[pl.ds(pl.multiple_of(me * rows, 8), rows)], own_sem)
    own.start()
    zero = (0,) * len(plan.dims)
    for stage in range(len(plan.dims)):
        for color, order in enumerate(plan.orders):
            moves = [m for m in plan.steps(zero, order) if m[0] == order[stage]]
            pass_on(color, piece(x_ref, 0, color), f, g, moves, [])
    if plan.core[1] == 2:
        for color in range(colors):
            remote(
                piece(x_ref, 0, color), buf, me * rows, color, side_send.at[color, seat(f, g)],
                side_recv.at[color, seat(f, g)], sibling,
            ).start()

    between()

    def owner_of(offset):
        owner_f, owner_g, conditions = f, g, []
        for d, (axis, stride, n) in enumerate(plan.dims):
            if not offset[d]:
                continue
            move = (1 - 2 * at[d]) if n == 2 else -offset[d]
            if n > 2:
                conditions.append(at[d] - offset[d] >= 0 if offset[d] > 0 else at[d] - offset[d] <= n - 1)
            if axis == "front":
                owner_f = owner_f + move * stride
            else:
                owner_g = owner_g + move * stride
        return owner_f, owner_g, conditions

    done = 0
    for number, (color, offset) in enumerate(plan.items):
        while done * len(plan.items) < number * len(chores):
            chores[done]()
            done += 1
        owner_f, owner_g, conditions = owner_of(offset)

        def arrive(color=color, offset=offset, owner_f=owner_f, owner_g=owner_g):
            first = (owner_f * plan.grid + owner_g) * rows
            here = piece(buf, first, color)
            remote(here, buf, first, color, send.at[0, color, seat(f, g)], recv.at[color, seat(owner_f, owner_g)], sibling).wait_recv()
            pass_on(color, here, owner_f, owner_g, plan.steps(offset, plan.orders[color]), conditions)
            if plan.core[1] == 2:
                remote(
                    here, buf, first, color, side_send.at[color, seat(owner_f, owner_g)],
                    side_recv.at[color, seat(owner_f, owner_g)], sibling,
                ).start()

        guarded(conditions, arrive)
    for chore in chores[done:]:
        chore()

    def finish():
        own.wait()
        everything = [(color, zero) for color in range(colors)] + plan.items
        for color, offset in everything:
            owner_f, owner_g, conditions = owner_of(offset)

            def settle(color=color, offset=offset, owner_f=owner_f, owner_g=owner_g):
                first = (owner_f * plan.grid + owner_g) * rows
                here = piece(buf, first, color)
                for d, step in plan.steps(offset, plan.orders[color]):
                    def gone(d=d, step=step):
                        remote(
                            here, buf, first, color, send.at[lane(d, step), color, seat(owner_f, owner_g)],
                            recv.at[color, seat(owner_f, owner_g)], moved(d, step),
                        ).wait_send()
                    guarded([inside(d, step)], gone)
                if plan.core[1] == 2:
                    remote(
                        here, buf, first, color, side_send.at[color, seat(owner_f, owner_g)],
                        side_recv.at[color, seat(owner_f, owner_g)], sibling,
                    ).wait_send()
                    theirs = ((owner_f + 1 - 2 * lax.rem(owner_f, 2)) * plan.grid + owner_g) * rows
                    remote(
                        piece(buf, theirs, color), buf, theirs, color, side_send.at[color, seat(owner_f, owner_g)],
                        side_recv.at[color, seat(owner_f, owner_g)], sibling,
                    ).wait_recv()

            guarded(conditions, settle)

    return finish


def greet(plan, everyone=False):
    f, g = lax.axis_index("front"), lax.axis_index("grid")
    bar = pltpu.get_barrier_semaphore()
    if everyone:
        total = plan.front * plan.grid
        me = f * plan.grid + g
        def hello(i, c):
            t = lax.rem(me + i, total)
            pl.semaphore_signal(bar, inc=1, device_id=(t // plan.grid, lax.rem(t, plan.grid)), device_id_type=MESH)
            return c
        lax.fori_loop(1, total, hello, 0)
        pl.semaphore_wait(bar, total - 1)


def ag_scratch(plan):
    seats = plan.front * plan.grid // plan.core[1]
    colors = len(plan.orders)
    return [
        pltpu.SemaphoreType.DMA(()),
        pltpu.SemaphoreType.DMA((2 * len(plan.dims), colors, seats)),
        pltpu.SemaphoreType.DMA((colors, seats)),
        pltpu.SemaphoreType.DMA((colors, seats)),
        pltpu.SemaphoreType.DMA((colors, seats)),
    ]


def halves(a):
    high = a.astype(jnp.bfloat16)
    return high, (a - high.astype(jnp.float32)).astype(jnp.bfloat16)


def dot(a, b):
    return jnp.dot(a, b, preferred_element_type=jnp.float32)


def add_product(acc, a_ref, high, low, tile):
    for m in range(a_ref.shape[0] // tile):
        rows = pl.ds(m * tile, tile)
        a_high, a_low = halves(a_ref[rows, :])
        acc[rows, :] += dot(a_high, high) + (dot(a_low, high) + dot(a_high, low))


def flat(block):
    return jnp.concatenate([block[:, 0, :], block[:, 1, :]], axis=1)


class Mail:
    def __init__(self, plan, rows, own_rows):
        self.plan, self.rows, self.own_rows = plan, rows, own_rows
        self.devices = plan.front * plan.grid
        mean = rows / self.devices
        self.slots = max(8, math.ceil((mean + 4.2 * math.sqrt(mean)) / 8) * 8)
        self.total = self.devices * self.slots
        self.parts = next(p for p in (4, 2, 1) if self.total % (16 * p) == 0)
        self.part = self.total // self.parts

    def scratch(self):
        return [
            pltpu.VMEM((self.devices, self.rows), jnp.float32),
            pltpu.VMEM((1, self.rows), jnp.float32),
            pltpu.VMEM((self.total, 1), jnp.float32),
            pltpu.VMEM((self.total, 256), jnp.float32),
            pltpu.VMEM((self.total, 256), jnp.float32),
            pltpu.SemaphoreType.DMA(()),
            pltpu.SemaphoreType.DMA((self.devices,)),
            pltpu.SemaphoreType.DMA((self.devices,)),
        ]

    def address(self, where, shift, peak, key, slot, target):
        n, rows, own = self.devices, self.rows, self.own_rows
        me = lax.axis_index("front") * self.plan.grid + lax.axis_index("grid")
        before = lax.broadcasted_iota(jnp.int32, (rows, rows), 0) < lax.broadcasted_iota(jnp.int32, (rows, rows), 1)
        before = jnp.where(before, 1.0, 0.0).astype(jnp.bfloat16)
        block = lax.broadcasted_iota(jnp.int32, (n, rows), 0)
        mine = where[pl.ds(me, 1), :]
        sent = (mine >= block * own) & (mine < (block + 1) * own)
        places = where[...] - me * own
        got = (places >= 0) & (places < own)
        both = jnp.concatenate([jnp.where(sent, 1.0, 0.0), jnp.where(got, 1.0, 0.0)], axis=0)
        rank = dot(both.astype(jnp.bfloat16), before) - shift
        own_rank, got_rank = rank[:n], rank[n:]
        fits = sent & (own_rank >= 0) & (own_rank < self.slots)
        number = (block * self.slots).astype(jnp.float32) + own_rank + 1.0
        slot[...] = jnp.sum(jnp.where(fits, number, 0.0), axis=0, keepdims=True) - 1.0
        key[...] = jnp.where(got, got_rank, -1.0)
        counter = lax.broadcasted_iota(jnp.int32, (self.slots, rows), 0).astype(jnp.float32)
        first = (block * own)

        def one(s, most):
            which = where[pl.ds(s, 1), :]
            held = counter == key[pl.ds(s, 1), :]
            place = (which - me * own + 1).astype(jnp.float32)
            found = jnp.sum(jnp.where(held, place, 0.0), axis=1, keepdims=True) - 1.0
            target[pl.ds(pl.multiple_of(s * self.slots, 8), self.slots), :] = found
            inside = (which >= first) & (which < first + own)
            return jnp.maximum(most, jnp.sum(jnp.where(inside, 1.0, 0.0), axis=1, keepdims=True))

        most = lax.fori_loop(0, n, one, jnp.zeros((n, 1), jnp.float32))
        if peak is not None:
            peak[0, 0] = jnp.max(most)

    def pack(self, slot, pair, out):
        def one(p, c):
            base = p * self.part
            ids = (lax.broadcasted_iota(jnp.int32, (self.part, self.rows), 0) + base).astype(jnp.float32)
            chosen = jnp.where(ids == slot[...], 1.0, 0.0).astype(jnp.bfloat16)
            both = dot(chosen, pair[...])
            out[pl.ds(pl.multiple_of(base, 8), self.part), :] = both[:, :256] + both[:, 256:]
            return c
        lax.fori_loop(0, self.parts, one, 0)

    def peer(self, i):
        me = lax.axis_index("front") * self.plan.grid + lax.axis_index("grid")
        return lax.rem(me + i, self.devices)

    def letter(self, i, out, inbox, sent, received):
        t = self.peer(i)
        me = self.peer(0)
        rows = lambda ref, b: ref.at[pl.ds(pl.multiple_of(b * self.slots, 8), self.slots)]
        return pltpu.make_async_remote_copy(
            src_ref=rows(out, t), dst_ref=rows(inbox, me), send_sem=sent.at[i],
            recv_sem=received.at[i], device_id=(t // self.plan.grid, lax.rem(t, self.plan.grid)),
            device_id_type=MESH,
        )

    def home(self, out, inbox, sem):
        me = self.peer(0)
        rows = lambda ref: ref.at[pl.ds(pl.multiple_of(me * self.slots, 8), self.slots)]
        return pltpu.make_async_copy(rows(out), rows(inbox), sem)

    def send(self, out, inbox, sem, sent, received):
        self.home(out, inbox, sem).start()

        def one(i, c):
            self.letter(i, out, inbox, sent, received).start()
            return c
        lax.fori_loop(1, self.devices, one, 0)

    def settle(self, out, inbox, sem, sent, received):
        def one(i, c):
            self.letter(i, out, inbox, sent, received).wait()
            return c
        lax.fori_loop(1, self.devices, one, 0)
        self.home(out, inbox, sem).wait()

    def unpack(self, target, inbox, acc):
        def one(p, c):
            rows = pl.ds(pl.multiple_of(p * self.part, 8), self.part)
            places = lax.broadcasted_iota(jnp.int32, (self.part, self.own_rows), 1).astype(jnp.float32)
            chosen = jnp.where(target[rows, :] == places, 1.0, 0.0).astype(jnp.bfloat16)
            pair = jnp.concatenate(halves(inbox[rows, :]), axis=1)
            both = lax.dot_general(chosen, pair, (((0,), (0,)), ((), ())), preferred_element_type=jnp.float32)
            acc[...] += both[:, :256] + both[:, 256:]
            return c
        lax.fori_loop(0, self.parts, one, 0)


def main_kernel(plan, mail, index, length, places, x, u_hbm, f_hbm, out, sample, peak, where_out, rows_all, x_rows, live,
                where, child_a, child_b, u_high, u_low, tiles, acc, tsem, wsem, wsend, wrecv, ssem, *more):
    ag, post = more[:5], more[5:]
    key, slot, target, outbox, inbox, msem, sent, received = post
    f, g = lax.axis_index("front"), lax.axis_index("grid")
    ring, tall, wide = tiles.shape
    rows, order = u_hbm.shape
    half = x.shape[1] // 2
    depth = child_a.shape[0]

    def tile_copy(source, n, across):
        r, k = n // across, lax.rem(n, across)
        s = lax.rem(n, ring)
        return pltpu.make_async_copy(
            source.at[pl.ds(pl.multiple_of(r * tall, 8), tall), pl.ds(pl.multiple_of(k * wide, 128), wide)],
            tiles.at[s], tsem.at[s],
        )

    u_across, f_across = order // wide, f_hbm.shape[1] // wide
    u_tiles, f_tiles = rows // tall * u_across, f_hbm.shape[0] // tall * f_across
    for n in range(ring):
        tile_copy(u_hbm, n, u_across).start()
    for h in range(2):
        x_rows[:, h, :] = x[:, h * half : (h + 1) * half]
    lane = lax.broadcasted_iota(jnp.int32, (1, rows), 1)
    for s in range(plan.grid):
        held = places[0:1, s * rows : (s + 1) * rows]
        live[s : s + 1, :] = jnp.where(lane + s * rows < length[0], held, -1)
    greet(plan, True)

    def here(ref, ff):
        return ref.at[pl.ds(pl.multiple_of(ff * plan.grid, 8), plan.grid)]

    def exchange(i):
        return pltpu.make_async_remote_copy(
            src_ref=live, dst_ref=here(where, f), send_sem=wsend.at[i], recv_sem=wrecv.at[i],
            device_id=(lax.rem(f + i, plan.front), g), device_id_type=MESH,
        )

    for i in range(1, plan.front):
        exchange(i).start()
    mine = pltpu.make_async_copy(live, here(where, f), wsem)
    mine.start()

    def between():
        for i in range(1, plan.front):
            exchange(i).wait()
        mine.wait()
        mail.address(where, 0.0, peak, key, slot, target)

    def f_copy(n):
        s = lax.rem(n + u_tiles, ring)
        r, k = n // f_across, lax.rem(n, f_across)
        return pltpu.make_async_copy(
            f_hbm.at[pl.ds(pl.multiple_of(r * tall, 8), tall), pl.ds(pl.multiple_of(k * wide, 128), wide)],
            tiles.at[s], tsem.at[s],
        )

    def split_tile(n):
        def chore():
            tile_copy(u_hbm, n, u_across).wait()
            r, k = n // u_across * tall, n % u_across * wide

            def some(i, c):
                first = pl.multiple_of(i * 32, 32)
                high, low = halves(tiles[n % ring, pl.ds(first, 32), :])
                u_high[pl.ds(r + first, 32), k : k + wide] = high
                u_low[pl.ds(r + first, 32), k : k + wide] = low
                return c

            lax.fori_loop(0, tall // 32, some, 0)
            if n + ring < u_tiles:
                tile_copy(u_hbm, n + ring, u_across).start()
            else:
                f_copy(n + ring - u_tiles).start()
        return chore

    finish = gather_rows(
        plan, x_rows, rows_all, *ag, between=between, chores=[split_tile(n) for n in range(u_tiles)]
    )
    finish()

    def fetch(child, k, first, count):
        for r in range(first, first + count):
            child[r] = rows_all[index[0, k * depth + r]]

    def multiply(child, k, following, ahead):
        high, low = halves(flat(child[...]))
        tile = min(256, rows)
        count = rows // tile
        columns = pl.ds(pl.multiple_of(k * depth, 128), depth)
        for m in range(count):
            part = pl.ds(m * tile, tile)
            a_high = u_high[part, columns]
            acc[part, :] += dot(a_high, high) + (dot(u_low[part, columns], high) + dot(a_high, low))
            fetch(following, ahead, m * depth // count, depth // count)

    acc[...] = jnp.zeros_like(acc)
    steps = order // depth

    def first_rows(j, c):
        for t in range(16):
            child_a[j * 16 + t] = rows_all[index[0, j * 16 + t]]
        return c

    lax.fori_loop(0, depth // 16, first_rows, 0)

    def two(j, c):
        multiply(child_a, 2 * j, child_b, 2 * j + 1)
        multiply(child_b, 2 * j + 1, child_a, lax.rem(2 * j + 2, steps))
        return c

    lax.fori_loop(0, steps // 2, two, 0)

    width = acc.shape[1]
    pair = u_high.at[:, pl.ds(0, 2 * width)]
    pair[...] = jnp.concatenate(halves(acc[...]), axis=1)
    mail.pack(slot, pair, outbox)
    keep = pltpu.make_async_copy(acc, sample, ssem)
    keep.start()
    mail.send(outbox, inbox, msem, sent, received)
    copy = pltpu.make_async_copy(where, where_out, wsem)
    copy.start()

    out[...] = jnp.zeros_like(out)

    def f_step(n, c):
        f_copy(n).wait()
        r, k = n // f_across, lax.rem(n, f_across)
        high, low = halves(flat(rows_all[pl.ds(pl.multiple_of(k * wide, wide), wide)]))
        add_product(out.at[pl.ds(pl.multiple_of(r * tall, 8), tall)], tiles.at[lax.rem(n + u_tiles, ring)], high, low, min(256, tall))

        @pl.when(n + ring < f_tiles)
        def _():
            f_copy(n + ring).start()

        return c

    lax.fori_loop(0, f_tiles, f_step, 0)

    mail.settle(outbox, inbox, msem, sent, received)
    mail.unpack(target, inbox, out)
    copy.wait()
    keep.wait()


def extra_kernel(plan, mail, shift, where, sample, so_far, out, pair2, *post):
    key, slot, target, outbox, inbox, msem, sent, received = post
    greet(plan, True)
    mail.address(where, shift[0:1, 0:1], None, key, slot, target)
    pair2[...] = jnp.concatenate(halves(sample[...]), axis=1)
    mail.pack(slot, pair2, outbox)
    mail.send(outbox, inbox, msem, sent, received)
    out[...] = so_far[...]
    mail.settle(outbox, inbox, msem, sent, received)
    mail.unpack(target, inbox, out)


def shards(plan, index_map, lengths, update_front, front_matrix, random):
    order, own_rows = index_map.shape[1], front_matrix.shape[0]
    rows, width = update_front.shape[1], random.shape[1]
    mail = Mail(plan, rows, own_rows)
    depth, ring, tall, wide = 512, 3, min(512, rows, own_rows), 512
    vmem, any_ = pl.BlockSpec(memory_space=pltpu.VMEM), pl.BlockSpec(memory_space=pl.ANY)
    smem = pl.BlockSpec(memory_space=pltpu.SMEM)
    devices = plan.front * plan.grid
    first, sample, peak, where = pl.pallas_call(
        functools.partial(main_kernel, plan, mail),
        out_shape=(
            jax.ShapeDtypeStruct((own_rows, width), jnp.float32),
            jax.ShapeDtypeStruct((rows, width), jnp.float32),
            jax.ShapeDtypeStruct((1, 1), jnp.float32),
            jax.ShapeDtypeStruct((devices, rows), jnp.int32),
        ),
        in_specs=[smem, smem, vmem, vmem, any_, any_],
        out_specs=(vmem, any_, smem, any_),
        scratch_shapes=[
            pltpu.VMEM((own_rows * devices, 2, width // 2), jnp.float32),
            pltpu.VMEM((own_rows, 2, width // 2), jnp.float32),
            pltpu.VMEM((plan.grid, rows), jnp.int32),
            pltpu.VMEM((devices, rows), jnp.int32),
            pltpu.VMEM((depth, 2, width // 2), jnp.float32),
            pltpu.VMEM((depth, 2, width // 2), jnp.float32),
            pltpu.VMEM((rows, order), jnp.bfloat16),
            pltpu.VMEM((rows, order), jnp.bfloat16),
            pltpu.VMEM((ring, tall, wide), jnp.float32),
            pltpu.VMEM((rows, width), jnp.float32),
            pltpu.SemaphoreType.DMA((ring,)),
            pltpu.SemaphoreType.DMA(()),
            pltpu.SemaphoreType.DMA((plan.front,)),
            pltpu.SemaphoreType.DMA((plan.front,)),
            pltpu.SemaphoreType.DMA(()),
            *ag_scratch(plan),
            *mail.scratch(),
        ],
        compiler_params=pltpu.CompilerParams(collective_id=0, has_side_effects=True, vmem_limit_bytes=67043328),
    )(index_map, lengths, index_map, random, update_front[0], front_matrix)

    def more(carry):
        done, so_far = carry
        shift = jnp.full((8, 128), done, jnp.float32)
        added = pl.pallas_call(
            functools.partial(extra_kernel, plan, mail),
            out_shape=jax.ShapeDtypeStruct((own_rows, width), jnp.float32),
            in_specs=[vmem] * 4,
            out_specs=vmem,
            scratch_shapes=[pltpu.VMEM((rows, 2 * width), jnp.bfloat16), *mail.scratch()],
            compiler_params=pltpu.CompilerParams(collective_id=1, has_side_effects=True, vmem_limit_bytes=63 << 20),
        )(shift, where, sample, so_far)
        return done + mail.slots, added

    return lax.while_loop(lambda carry: carry[0] < peak[0, 0], more, (jnp.float32(mail.slots), first))[1]


def solution(mesh):
    plan = Plan(mesh)
    placed = (
        P("front", None),
        P("front"),
        P("front", "grid", None),
        P(("front", "grid"), None),
        P(("front", "grid"), None),
    )
    return jax.shard_map(
        functools.partial(shards, plan), mesh=mesh, in_specs=placed, out_specs=P(("front", "grid"), None),
        check_vma=False,
    )
```

```python
import functools
import itertools
import math

import jax
import jax.numpy as jnp
from jax import lax
from jax.experimental import pallas as pl
from jax.experimental.pallas import tpu as pltpu
from jax.sharding import PartitionSpec as P

MESH = pl.DeviceIdType.MESH


def axis_dims(places):
    found = []
    for d in range(len(places[0])):
        values = [p[d] for p in places]
        size = len(set(values))
        if size > 1:
            stride = next(i for i, v in enumerate(values) if v != values[0])
            found.append((stride, size))
    found.sort(reverse=True)
    if math.prod(size for _, size in found) != len(places):
        found = [(1, len(places))]
    return found


class Plan:
    def __init__(self, mesh):
        self.front, self.grid = mesh.shape["front"], mesh.shape["grid"]
        place = lambda d: (*d.coords, d.core_on_chip)
        fronts = axis_dims([place(d) for d in mesh.devices[:, 0]])
        grids = axis_dims([place(d) for d in mesh.devices[0, :]])
        self.core = fronts[-1] if fronts[-1][1] == 2 else (1, 1)
        if self.core[1] == 2:
            fronts = fronts[:-1]
        dims = [("front", s, n) for s, n in fronts] + [("grid", s, n) for s, n in grids]
        long = max(range(len(dims)), key=lambda i: dims[i][2])
        rest = [i for i in range(len(dims)) if i != long]
        self.dims = dims
        a, b = rest, rest[::-1]
        if len(rest) == 2:
            self.orders = [[(a[0], long, a[1]), (long, *b)], [(b[0], long, b[1]), (long, *a)]]
        else:
            self.orders = [[(*a, long), (long, *b)], [(*b, long), (long, *a)]]
        self.lanes, self.lane_count = {}, 0
        for d, (_, _, n) in enumerate(dims):
            for step in (1,) if n == 2 else (1, -1):
                self.lanes[d, step] = self.lane_count
                self.lane_count += 1
        self.items = [self.schedule(h) for h in range(2)]

    def steps(self, offset, order):
        last = max((i for i, d in enumerate(order) if offset[d]), default=-1)
        moves = []
        if last >= 0 and self.dims[order[last]][2] > 2:
            moves.append((order[last], 1 if offset[order[last]] > 0 else -1))
        for d in order[last + 1 :]:
            moves += [(d, 1)] if self.dims[d][2] == 2 else [(d, 1), (d, -1)]
        return moves

    def schedule(self, h):
        spans = [range(2) if n == 2 else range(1 - n, n) for _, _, n in self.dims]
        items = []
        for offset in itertools.product(*spans):
            for color, order in enumerate(self.orders[h]):
                stage = max((i for i, d in enumerate(order) if offset[d]), default=-1)
                items.append((sum(map(abs, offset)), stage, color, offset))
        items.sort()
        return [(color, offset) for hops, _, color, offset in items if hops]


class Gather:
    def __init__(self, plan, x_ref, buf, own_sem, send, side_send, recv, side_recv):
        self.plan, self.x_ref, self.buf, self.own_sem = plan, x_ref, buf, own_sem
        self.send, self.side_send, self.recv, self.side_recv = send, side_send, recv, side_recv
        self.f, self.g = f, g = lax.axis_index("front"), lax.axis_index("grid")
        self.rows, self.width = x_ref.shape[0], buf[0].shape[1]
        self.colors = len(plan.orders[0])
        self.part = self.rows // self.colors
        self.at = [lax.rem((f if axis == "front" else g) // s, n) for axis, s, n in plan.dims]
        self.sibling = (f + 1 - 2 * lax.rem(f, 2), g)
        self.zero = (0,) * len(plan.dims)

    def moved(self, d, step):
        axis, stride, n = self.plan.dims[d]
        move = (1 - 2 * self.at[d]) if n == 2 else step
        return (self.f + move * stride, self.g) if axis == "front" else (self.f, self.g + move * stride)

    def inside(self, d, step):
        n = self.plan.dims[d][2]
        if n == 2:
            return None
        return self.at[d] + step <= n - 1 if step > 0 else self.at[d] + step >= 0

    def guarded(self, conditions, body):
        conditions = [c for c in conditions if c is not None]
        if conditions:
            pl.when(functools.reduce(jnp.logical_and, conditions))(body)
        else:
            body()

    def here(self, owner_f, owner_g, h, color):
        first = (owner_f * self.plan.grid + owner_g) * self.rows + color * self.part
        return self.buf[h].at[pl.ds(pl.multiple_of(first, 8), self.part)]

    def given(self, h, color):
        return self.x_ref.at[pl.ds(color * self.part, self.part), pl.ds(h * self.width, self.width)]

    def seat(self, owner_f, owner_g):
        return (owner_f // self.plan.core[1]) * self.plan.grid + owner_g

    def hop(self, source, owner_f, owner_g, h, color, d, step):
        seat = self.seat(owner_f, owner_g)
        return pltpu.make_async_remote_copy(
            src_ref=source, dst_ref=self.here(owner_f, owner_g, h, color),
            send_sem=self.send.at[h, self.plan.lanes[d, step], color, seat], recv_sem=self.recv.at[h, color, seat],
            device_id=self.moved(d, step), device_id_type=MESH,
        )

    def aside(self, source, owner_f, owner_g, h, color):
        seat = self.seat(owner_f, owner_g)
        return pltpu.make_async_remote_copy(
            src_ref=source, dst_ref=self.here(owner_f, owner_g, h, color), send_sem=self.side_send.at[h, color, seat],
            recv_sem=self.side_recv.at[h, color, seat], device_id=self.sibling, device_id_type=MESH,
        )

    def pass_on(self, source, owner_f, owner_g, h, color, moves):
        for d, step in moves:
            self.guarded([self.inside(d, step)], self.hop(source, owner_f, owner_g, h, color, d, step).start)

    def own(self, h):
        block = pl.ds(pl.multiple_of((self.f * self.plan.grid + self.g) * self.rows, 8), self.rows)
        return pltpu.make_async_copy(
            self.x_ref.at[:, pl.ds(h * self.width, self.width)], self.buf[h].at[block], self.own_sem.at[h]
        )

    def begin(self, h):
        self.own(h).start()
        for stage in range(len(self.plan.dims)):
            for color, order in enumerate(self.plan.orders[h]):
                moves = [m for m in self.plan.steps(self.zero, order) if m[0] == order[stage]]
                self.pass_on(self.given(h, color), self.f, self.g, h, color, moves)
        if self.plan.core[1] == 2:
            for color in range(self.colors):
                self.aside(self.given(h, color), self.f, self.g, h, color).start()

    def owner_of(self, offset):
        owner_f, owner_g, conditions = self.f, self.g, []
        for d, (axis, stride, n) in enumerate(self.plan.dims):
            if not offset[d]:
                continue
            move = (1 - 2 * self.at[d]) if n == 2 else -offset[d]
            if n > 2:
                conditions.append(self.at[d] >= offset[d] if offset[d] > 0 else self.at[d] - offset[d] <= n - 1)
            if axis == "front":
                owner_f = owner_f + move * stride
            else:
                owner_g = owner_g + move * stride
        return owner_f, owner_g, conditions

    def arrive(self, h, color, offset):
        owner_f, owner_g, conditions = self.owner_of(offset)

        def body():
            here = self.here(owner_f, owner_g, h, color)
            self.hop(here, owner_f, owner_g, h, color, 0, 1).wait_recv()
            self.pass_on(here, owner_f, owner_g, h, color, self.plan.steps(offset, self.plan.orders[h][color]))
            if self.plan.core[1] == 2:
                self.aside(here, owner_f, owner_g, h, color).start()

        self.guarded(conditions, body)

    def every(self, h, body):
        for color, offset in [(color, self.zero) for color in range(self.colors)] + self.plan.items[h]:
            owner_f, owner_g, conditions = self.owner_of(offset)
            self.guarded(conditions, functools.partial(body, h, color, offset, owner_f, owner_g))

    def complete(self, h):
        self.own(h).wait()

        def body(h, color, offset, owner_f, owner_g):
            theirs = owner_f + 1 - 2 * lax.rem(owner_f, 2)
            self.aside(self.here(theirs, owner_g, h, color), theirs, owner_g, h, color).wait_recv()

        if self.plan.core[1] == 2:
            self.every(h, body)

    def drain(self, h):
        def body(h, color, offset, owner_f, owner_g):
            here = self.here(owner_f, owner_g, h, color)
            for d, step in self.plan.steps(offset, self.plan.orders[h][color]):
                self.guarded([self.inside(d, step)], self.hop(here, owner_f, owner_g, h, color, d, step).wait_send)
            if self.plan.core[1] == 2:
                self.aside(here, owner_f, owner_g, h, color).wait_send()

        self.every(h, body)


def greet(plan, everyone=False):
    f, g = lax.axis_index("front"), lax.axis_index("grid")
    bar = pltpu.get_barrier_semaphore()
    if everyone:
        total = plan.front * plan.grid
        me = f * plan.grid + g
        def hello(i, c):
            t = lax.rem(me + i, total)
            pl.semaphore_signal(bar, inc=1, device_id=(t // plan.grid, lax.rem(t, plan.grid)), device_id_type=MESH)
            return c
        lax.fori_loop(1, total, hello, 0)
        pl.semaphore_wait(bar, total - 1)


def ag_scratch(plan):
    seats = plan.front * plan.grid // plan.core[1]
    colors = len(plan.orders[0])
    return [
        pltpu.SemaphoreType.DMA((2,)),
        pltpu.SemaphoreType.DMA((2, plan.lane_count, colors, seats)),
        pltpu.SemaphoreType.DMA((2, colors, seats)),
        pltpu.SemaphoreType.DMA((2, colors, seats)),
        pltpu.SemaphoreType.DMA((2, colors, seats)),
    ]


def halves(a):
    high = a.astype(jnp.bfloat16)
    return high, (a - high.astype(jnp.float32)).astype(jnp.bfloat16)


def dot(a, b):
    return jnp.dot(a, b, preferred_element_type=jnp.float32)


def add_product(acc, a_ref, high, low, tile):
    for m in range(a_ref.shape[0] // tile):
        rows = pl.ds(m * tile, tile)
        a_high, a_low = halves(a_ref[rows, :])
        acc[rows, :] += dot(a_high, high) + (dot(a_low, high) + dot(a_high, low))


class Mail:
    def __init__(self, plan, rows, own_rows, width):
        self.plan, self.rows, self.own_rows, self.width = plan, rows, own_rows, width
        self.devices = plan.front * plan.grid
        mean = rows / self.devices
        self.slots = max(8, math.ceil((mean + 4.2 * math.sqrt(mean)) / 8) * 8)
        self.total = self.devices * self.slots
        self.parts = next(p for p in (4, 2, 1) if self.total % (16 * p) == 0)
        self.part = self.total // self.parts

    def scratch(self):
        return [
            pltpu.VMEM((self.devices, self.rows), jnp.float32),
            pltpu.VMEM((1, self.rows), jnp.float32),
            pltpu.VMEM((self.total, 1), jnp.float32),
            pltpu.VMEM((2, self.total, self.width), jnp.float32),
            pltpu.VMEM((2, self.total, self.width), jnp.float32),
            pltpu.SemaphoreType.DMA((2,)),
            pltpu.SemaphoreType.DMA((2, self.devices)),
            pltpu.SemaphoreType.DMA((2, self.devices)),
        ]

    def address(self, where, shift, peak, key, slot, target):
        n, rows, own = self.devices, self.rows, self.own_rows
        me = lax.axis_index("front") * self.plan.grid + lax.axis_index("grid")
        before = lax.broadcasted_iota(jnp.int32, (rows, rows), 0) < lax.broadcasted_iota(jnp.int32, (rows, rows), 1)
        before = jnp.where(before, 1.0, 0.0).astype(jnp.bfloat16)
        block = lax.broadcasted_iota(jnp.int32, (n, rows), 0)
        mine = where[pl.ds(me, 1), :]
        sent = (mine >= block * own) & (mine < (block + 1) * own)
        places = where[...] - me * own
        got = (places >= 0) & (places < own)
        both = jnp.concatenate([jnp.where(sent, 1.0, 0.0), jnp.where(got, 1.0, 0.0)], axis=0)
        rank = dot(both.astype(jnp.bfloat16), before) - shift
        own_rank, got_rank = rank[:n], rank[n:]
        fits = sent & (own_rank >= 0) & (own_rank < self.slots)
        number = (block * self.slots).astype(jnp.float32) + own_rank + 1.0
        slot[...] = jnp.sum(jnp.where(fits, number, 0.0), axis=0, keepdims=True) - 1.0
        key[...] = jnp.where(got, got_rank, -1.0)
        counter = lax.broadcasted_iota(jnp.int32, (self.slots, rows), 0).astype(jnp.float32)
        first = (block * own)

        def one(s, most):
            which = where[pl.ds(s, 1), :]
            held = counter == key[pl.ds(s, 1), :]
            place = (which - me * own + 1).astype(jnp.float32)
            found = jnp.sum(jnp.where(held, place, 0.0), axis=1, keepdims=True) - 1.0
            target[pl.ds(pl.multiple_of(s * self.slots, 8), self.slots), :] = found
            inside = (which >= first) & (which < first + own)
            return jnp.maximum(most, jnp.sum(jnp.where(inside, 1.0, 0.0), axis=1, keepdims=True))

        most = lax.fori_loop(0, n, one, jnp.zeros((n, 1), jnp.float32))
        if peak is not None:
            peak[0, 0] = jnp.max(most)

    def pack(self, slot, pair, out):
        def one(p, c):
            base = p * self.part
            ids = (lax.broadcasted_iota(jnp.int32, (self.part, self.rows), 0) + base).astype(jnp.float32)
            chosen = jnp.where(ids == slot[...], 1.0, 0.0).astype(jnp.bfloat16)
            both = dot(chosen, pair[...])
            out[pl.ds(pl.multiple_of(base, 8), self.part), :] = both[:, : self.width] + both[:, self.width :]
            return c
        lax.fori_loop(0, self.parts, one, 0)

    def peer(self, i):
        me = lax.axis_index("front") * self.plan.grid + lax.axis_index("grid")
        return lax.rem(me + i, self.devices)

    def letter(self, h, i, out, inbox, sent, received):
        t = self.peer(i)
        me = self.peer(0)
        rows = lambda ref, b: ref.at[h, pl.ds(pl.multiple_of(b * self.slots, 8), self.slots)]
        return pltpu.make_async_remote_copy(
            src_ref=rows(out, t), dst_ref=rows(inbox, me), send_sem=sent.at[h, i],
            recv_sem=received.at[h, i], device_id=(t // self.plan.grid, lax.rem(t, self.plan.grid)),
            device_id_type=MESH,
        )

    def home(self, h, out, inbox, sem):
        me = self.peer(0)
        rows = lambda ref: ref.at[h, pl.ds(pl.multiple_of(me * self.slots, 8), self.slots)]
        return pltpu.make_async_copy(rows(out), rows(inbox), sem.at[h])

    def send(self, h, out, inbox, sem, sent, received):
        self.home(h, out, inbox, sem).start()

        def one(i, c):
            self.letter(h, i, out, inbox, sent, received).start()
            return c
        lax.fori_loop(1, self.devices, one, 0)

    def settle(self, h, out, inbox, sem, sent, received):
        def one(i, c):
            self.letter(h, i, out, inbox, sent, received).wait()
            return c
        lax.fori_loop(1, self.devices, one, 0)
        self.home(h, out, inbox, sem).wait()

    def unpack(self, target, inbox, acc):
        def one(p, c):
            rows = pl.ds(pl.multiple_of(p * self.part, 8), self.part)
            places = lax.broadcasted_iota(jnp.int32, (self.part, self.own_rows), 1).astype(jnp.float32)
            chosen = jnp.where(target[rows, :] == places, 1.0, 0.0).astype(jnp.bfloat16)
            pair = jnp.concatenate(halves(inbox[rows, :]), axis=1)
            both = lax.dot_general(chosen, pair, (((0,), (0,)), ((), ())), preferred_element_type=jnp.float32)
            acc[...] += both[:, : self.width] + both[:, self.width :]
            return c
        lax.fori_loop(0, self.parts, one, 0)


def main_kernel(plan, mail, index, length, places, x, u_hbm, f_hbm, out, sample, peak, where_out, rows_0, rows_1, live,
                where, child, both, u_high, u_low, tiles, acc, product, pair, tsem, wsem, wsend, wrecv, ssem, *more):
    ag, post = more[:5], more[5:]
    key, slot, target, outbox, inbox, msem, sent, received = post
    f, g = lax.axis_index("front"), lax.axis_index("grid")
    ring, tall, wide = tiles.shape
    rows, order = u_hbm.shape
    rows_all = (rows_0, rows_1)
    width = rows_0.shape[1]
    depth = child.shape[0]
    gather = Gather(plan, x, rows_all, *ag)

    def tile_copy(source, n, across):
        r, k = n // across, n % across
        s = n % ring
        return pltpu.make_async_copy(
            source.at[pl.ds(r * tall, tall), pl.ds(k * wide, wide)], tiles.at[s], tsem.at[s]
        )

    u_across, f_across = order // wide, f_hbm.shape[1] // wide
    u_tiles, f_tiles = rows // tall * u_across, f_hbm.shape[0] // tall * f_across
    for n in range(ring):
        tile_copy(u_hbm, n, u_across).start()
    lane = lax.broadcasted_iota(jnp.int32, (1, rows), 1)
    for s in range(plan.grid):
        held = places[0:1, s * rows : (s + 1) * rows]
        live[s : s + 1, :] = jnp.where(lane + s * rows < length[0], held, -1)
    greet(plan, True)
    gather.begin(0)

    def here(ref, ff):
        return ref.at[pl.ds(pl.multiple_of(ff * plan.grid, 8), plan.grid)]

    def exchange(i):
        return pltpu.make_async_remote_copy(
            src_ref=live, dst_ref=here(where, f), send_sem=wsend.at[i], recv_sem=wrecv.at[i],
            device_id=(lax.rem(f + i, plan.front), g), device_id_type=MESH,
        )

    for i in range(1, plan.front):
        exchange(i).start()
    mine = pltpu.make_async_copy(live, here(where, f), wsem)
    mine.start()

    def f_copy(n):
        s = lax.rem(n + u_tiles, ring)
        r, k = n // f_across, lax.rem(n, f_across)
        return pltpu.make_async_copy(
            f_hbm.at[pl.ds(pl.multiple_of(r * tall, 8), tall), pl.ds(pl.multiple_of(k * wide, 128), wide)],
            tiles.at[s], tsem.at[s],
        )

    def split_tile(n):
        def chore():
            tile_copy(u_hbm, n, u_across).wait()
            r, k = n // u_across * tall, n % u_across * wide

            def some(i, c):
                first = pl.multiple_of(i * 32, 32)
                high, low = halves(tiles[n % ring, pl.ds(first, 32), :])
                u_high[pl.ds(r + first, 32), k : k + wide] = high
                u_low[pl.ds(r + first, 32), k : k + wide] = low
                return c

            lax.fori_loop(0, tall // 32, some, 0)
            if n + ring < u_tiles:
                tile_copy(u_hbm, n + ring, u_across).start()
            else:
                f_copy(n + ring - u_tiles).start()
        return chore

    def address():
        for i in range(1, plan.front):
            exchange(i).wait()
        mine.wait()
        mail.address(where, 0.0, peak, key, slot, target)
        pltpu.make_async_copy(where, where_out, wsem).start()

    steps = order // depth
    block = min(256, rows)
    blocks = rows // block

    def first_rows(h):
        def some(j, c):
            for t in range(16):
                child[pl.ds(j * 16 + t, 1), :] = rows_all[h][pl.ds(index[0, j * 16 + t], 1), :]
            return c
        lax.fori_loop(0, depth // 16, some, 0)

    def multiply(h, k):
        high, low = halves(child[...])
        both[:, :width] = high
        both[:, width:] = low
        columns = pl.ds(pl.multiple_of(k * depth, 128), depth)
        ahead = lax.rem(k + 1, steps) * depth
        count = depth // blocks
        for m in range(blocks):
            part = pl.ds(m * block, block)
            first = dot(u_high[part, columns], both[...])
            second = dot(u_low[part, columns], both[:, :width])
            acc[part, width:] += first[:, width:]
            acc[part, :width] += first[:, :width] + second
            for r in range(m * count, (m + 1) * count):
                child[pl.ds(r, 1), :] = rows_all[h][pl.ds(index[0, ahead + r], 1), :]

    def start_half(h):
        acc[...] = jnp.zeros_like(acc)
        first_rows(h)

    def keep(h):
        return pltpu.make_async_copy(product.at[h], sample.at[h], ssem.at[h])

    def post_half(h):
        product[h] = acc[:, :width] + acc[:, width:]
        high, low = halves(product[h])
        pair[:, :width] = high
        pair[:, width:] = low
        mail.pack(slot, pair, outbox.at[h])
        keep(h).start()
        mail.send(h, outbox, inbox, msem, sent, received)

    def run(h, chores):
        done = 0
        items = plan.items[h]
        for number, (color, offset) in enumerate(items):
            while done * len(items) < number * len(chores):
                chores[done]()
                done += 1
            gather.arrive(h, color, offset)
        for chore in chores[done:]:
            chore()

    chores = [address] + [split_tile(n) for n in range(u_tiles)]
    chores.insert(len(chores) * 3 // 4, lambda: gather.begin(1))
    run(0, chores)
    gather.complete(0)
    start_half(0)
    run(1, [functools.partial(multiply, 0, k) for k in range(steps)])
    post_half(0)
    gather.complete(1)
    start_half(1)

    def step(k, c):
        multiply(1, k)
        return c

    lax.fori_loop(0, steps, step, 0)
    post_half(1)

    out[...] = jnp.zeros_like(out)

    def f_step(n, c):
        f_copy(n).wait()
        r, k = n // f_across, lax.rem(n, f_across)
        at = pl.ds(pl.multiple_of(k * wide, wide), wide)
        high, low = halves(jnp.concatenate([rows_0[at, :], rows_1[at, :]], axis=1))
        add_product(out.at[pl.ds(pl.multiple_of(r * tall, 8), tall)], tiles.at[lax.rem(n + u_tiles, ring)], high, low, min(256, tall))

        @pl.when(n + ring < f_tiles)
        def _():
            f_copy(n + ring).start()

        return c

    lax.fori_loop(0, f_tiles, f_step, 0)
    gather.drain(0)
    gather.drain(1)
    for h in range(2):
        mail.settle(h, outbox, inbox, msem, sent, received)
        mail.unpack(target, inbox.at[h], out.at[:, pl.ds(h * width, width)])
    pltpu.make_async_copy(where, where_out, wsem).wait()
    for h in range(2):
        keep(h).wait()


def extra_kernel(plan, mail, shift, where, sample, so_far, out, pair, *post):
    key, slot, target, outbox, inbox, msem, sent, received = post
    width = mail.width
    greet(plan, True)
    mail.address(where, shift[0:1, 0:1], None, key, slot, target)
    for h in range(2):
        high, low = halves(sample[h])
        pair[:, :width] = high
        pair[:, width:] = low
        mail.pack(slot, pair, outbox.at[h])
        mail.send(h, outbox, inbox, msem, sent, received)
    out[...] = so_far[...]
    for h in range(2):
        mail.settle(h, outbox, inbox, msem, sent, received)
        mail.unpack(target, inbox.at[h], out.at[:, pl.ds(h * width, width)])


def shards(plan, index_map, lengths, update_front, front_matrix, random):
    order, own_rows = index_map.shape[1], front_matrix.shape[0]
    rows, width = update_front.shape[1], random.shape[1]
    half = width // 2
    mail = Mail(plan, rows, own_rows, half)
    depth, ring, tall, wide = 512, 3, min(512, rows, own_rows), 512
    vmem, any_ = pl.BlockSpec(memory_space=pltpu.VMEM), pl.BlockSpec(memory_space=pl.ANY)
    smem = pl.BlockSpec(memory_space=pltpu.SMEM)
    devices = plan.front * plan.grid
    first, sample, peak, where = pl.pallas_call(
        functools.partial(main_kernel, plan, mail),
        out_shape=(
            jax.ShapeDtypeStruct((own_rows, width), jnp.float32),
            jax.ShapeDtypeStruct((2, rows, half), jnp.float32),
            jax.ShapeDtypeStruct((1, 1), jnp.float32),
            jax.ShapeDtypeStruct((devices, rows), jnp.int32),
        ),
        in_specs=[smem, smem, vmem, vmem, any_, any_],
        out_specs=(vmem, any_, smem, any_),
        scratch_shapes=[
            pltpu.VMEM((own_rows * devices, half), jnp.float32),
            pltpu.VMEM((own_rows * devices, half), jnp.float32),
            pltpu.VMEM((plan.grid, rows), jnp.int32),
            pltpu.VMEM((devices, rows), jnp.int32),
            pltpu.VMEM((depth, half), jnp.float32),
            pltpu.VMEM((depth, width), jnp.bfloat16),
            pltpu.VMEM((rows, order), jnp.bfloat16),
            pltpu.VMEM((rows, order), jnp.bfloat16),
            pltpu.VMEM((ring, tall, wide), jnp.float32),
            pltpu.VMEM((rows, width), jnp.float32),
            pltpu.VMEM((2, rows, half), jnp.float32),
            pltpu.VMEM((rows, width), jnp.bfloat16),
            pltpu.SemaphoreType.DMA((ring,)),
            pltpu.SemaphoreType.DMA(()),
            pltpu.SemaphoreType.DMA((plan.front,)),
            pltpu.SemaphoreType.DMA((plan.front,)),
            pltpu.SemaphoreType.DMA((2,)),
            *ag_scratch(plan),
            *mail.scratch(),
        ],
        compiler_params=pltpu.CompilerParams(collective_id=0, has_side_effects=True, vmem_limit_bytes=67043328),
    )(index_map, lengths, index_map, random, update_front[0], front_matrix)

    def more(carry):
        done, so_far = carry
        shift = jnp.full((8, 128), done, jnp.float32)
        added = pl.pallas_call(
            functools.partial(extra_kernel, plan, mail),
            out_shape=jax.ShapeDtypeStruct((own_rows, width), jnp.float32),
            in_specs=[vmem] * 4,
            out_specs=vmem,
            scratch_shapes=[pltpu.VMEM((rows, width), jnp.bfloat16), *mail.scratch()],
            compiler_params=pltpu.CompilerParams(collective_id=1, has_side_effects=True, vmem_limit_bytes=63 << 20),
        )(shift, where, sample, so_far)
        return done + mail.slots, added

    return lax.while_loop(lambda carry: carry[0] < peak[0, 0], more, (jnp.float32(mail.slots), first))[1]


def solution(mesh):
    plan = Plan(mesh)
    placed = (
        P("front", None),
        P("front"),
        P("front", "grid", None),
        P(("front", "grid"), None),
        P(("front", "grid"), None),
    )
    return jax.shard_map(
        functools.partial(shards, plan), mesh=mesh, in_specs=placed, out_specs=P(("front", "grid"), None),
        check_vma=False,
    )
```
